32 devices in a mesh: dp: 4 (over x, core), fsdp: 4 (over z), tp: 2 (over y).
Axes of the slice: x: 2, y: 2, z: 4, core: 2. Of those that a mesh axis runs over, the one named last changes fastest.
Arguments:
- hidden: bfloat16 [8192, 7168], P(('dp', 'fsdp')), may hold values from -6 to 6
- cotangent: bfloat16 [8192, 576], P(('dp', 'fsdp'), 'tp'), may hold values from -6 to 6
- rewards: int32 [64], P(('dp', 'fsdp')), may hold values from 0 to 8
- groups: int32 [64], P(('dp', 'fsdp')), may hold values from 0 to 3, as said below
- lengths: int32 [64], P(('dp', 'fsdp')), may hold values from 1 to 128
- master: float32 [4, 1792, 576], P('fsdp', 'dp', 'tp'), may hold values from -6 to 6
Outputs:
- grad_owned: float32 [4, 1792, 576], P('fsdp', 'dp', 'tp')
- rollout: bfloat16 [4, 1792, 576], P('fsdp')
The draws below stay inside these ranges and needn't reach their ends.
Inputs may be any that keep to these rules, and one draw needn't show every extreme that they name: `groups`: each prompt number names exactly 16 samples.
All inputs are finite; a program needn't handle non-finite values.
Results may differ from the reference program's by a relative error of at most 0.0033.
Values may be sent and summed in bfloat16 or wider, within the bound.
A program may use at most 64 MiB of HBM per device.

```python
import jax
import jax.numpy as jnp
from jax import lax

D = 7168
R = 576
GROUP = 16
SEQ = 128
TOK_DEV = 512
SAMPLES = 64
TOKENS = 8192
GROUPS = 4
N_FSDP = 4


def draw_groups(key, part):
    order = jax.random.permutation(jax.random.fold_in(key, 7), SAMPLES)
    return (order // GROUP).astype(jnp.int32)


def plant(entries, stream_key, least, high):
    shape = entries.shape
    index_at = [jax.random.randint(jax.random.fold_in(stream_key, axis), (), 0, shape[axis]) for axis in range(len(shape))]
    entries = entries.at[tuple(index_at)].set(least)
    longest = shape.index(max(shape))
    index_at[longest] = (index_at[longest] + 1) % shape[longest]
    return entries.at[tuple(index_at)].set(high)


def levels(own_key, shape, split, low, largest):
    def one(axis_at, parts):
        steps = jax.random.uniform(jax.random.fold_in(jax.random.fold_in(own_key, 6), axis_at), (parts,), jnp.float32, low / len(split), largest / len(split))
        return jnp.repeat(jnp.exp(steps), shape[axis_at] // parts).reshape((-1,) + (1,) * (len(shape) - axis_at - 1))

    loudness = one(*split[0])
    for cut in split[1:]:
        loudness = loudness * one(*cut)
    return loudness


def scatter_about(own_key, extent, scale, bound, shards=(), kind=jnp.bfloat16):
    result = scale * jax.random.normal(own_key, extent, jnp.float32)
    if shards:
        result = result * levels(own_key, extent, shards, -0.22, 0.18)
    return jnp.clip(result, -bound, bound).astype(kind)


def setup_inputs(seed: int = 0) -> dict:
    splits = jax.random.split(jax.random.key(seed), 7)
    return {
        "hidden": scatter_about(splits[0], (TOKENS, D), 1.0, 6.0, ((0, 16),)),
        "cotangent": scatter_about(splits[1], (TOKENS, R), 1.0, 6.0, ((0, 16), (1, 2))),
        "rewards": plant(jax.random.randint(splits[2], (SAMPLES,), 0, 9), jax.random.fold_in(splits[2], 1), 0, 8).astype(jnp.int32),
        "groups": draw_groups(jax.random.fold_in(splits[6], 71), 0),
        "lengths": plant(jax.random.randint(splits[4], (SAMPLES,), 1, SEQ + 1), jax.random.fold_in(splits[4], 1), 1, SEQ).astype(jnp.int32),
        "master": scatter_about(splits[5], (N_FSDP, D // N_FSDP, R), 1.0, 6.0, ((0, 4), (1, 4), (2, 2)), jnp.float32),
    }


def reference(hidden, cotangent, rewards, groups, lengths, master):
    labels = jnp.arange(GROUPS, dtype=jnp.int32)
    onehot = (groups[:, None] == labels[None, :]).astype(jnp.float32)
    reward_f = rewards.astype(jnp.float32)
    totals = jnp.dot(reward_f, onehot, precision=lax.Precision.HIGHEST)
    squares = jnp.dot(reward_f * reward_f, onehot, precision=lax.Precision.HIGHEST)
    group_mean = totals / GROUP
    group_square = squares / GROUP
    sample_mean = jnp.dot(onehot, group_mean, precision=lax.Precision.HIGHEST)
    sample_square = jnp.dot(onehot, group_square, precision=lax.Precision.HIGHEST)
    advantage = (reward_f - sample_mean) / jnp.sqrt(sample_square - sample_mean * sample_mean + 1.0)
    positions = jnp.arange(SEQ, dtype=jnp.int32)
    live = (positions[None, :] < lengths[:, None]).astype(jnp.float32)
    scale = (advantage[:, None] * live / lengths[:, None].astype(jnp.float32)).reshape(TOKENS)
    weighted = (cotangent.astype(jnp.float32) * scale[:, None]).astype(jnp.bfloat16)
    blocks = TOKENS // TOK_DEV
    hidden_blocks = hidden.reshape(blocks, TOK_DEV, D)
    weighted_blocks = weighted.reshape(blocks, TOK_DEV, R)

    def add_block(carry, pair):
        left = pair[0].astype(jnp.float32)
        right = pair[1].astype(jnp.float32)
        return (carry + jnp.dot(left.T, right, precision=lax.Precision.HIGHEST), None)
    grad, _ = lax.scan(add_block, jnp.zeros((D, R), jnp.float32), (hidden_blocks, weighted_blocks))
    grad_owned = grad.reshape(N_FSDP, D // N_FSDP, R)
    rollout = (master - 0.1 * grad_owned).astype(jnp.bfloat16)
    return (grad_owned, rollout)
```

```python
import functools

import jax
import jax.numpy as jnp
from jax import lax
from jax.experimental import pallas as pl
from jax.experimental.pallas import tpu as pltpu
from jax.sharding import PartitionSpec as P

D = 7168
GROUP = 16


def exact_dot(left, right):
    return jnp.dot(left, right, precision=lax.Precision.HIGHEST)


def shards(hidden, cotangent, rewards, groups, lengths, master):
    fsdp_size = lax.axis_size("fsdp")
    dp_size = lax.axis_size("dp")
    samp_local = rewards.shape[0]
    group_count = samp_local * dp_size * fsdp_size // GROUP
    labels = jnp.arange(group_count, dtype=jnp.int32)
    reward_f = rewards.astype(jnp.float32)
    local_onehot = (groups[:, None] == labels[None, :]).astype(jnp.float32)
    totals, squares = lax.psum(
        (exact_dot(reward_f, local_onehot), exact_dot(reward_f * reward_f, local_onehot)),
        ("dp", "fsdp"),
    )
    group_mean = totals / GROUP
    group_square = squares / GROUP
    sample_mean = exact_dot(local_onehot, group_mean)
    sample_square = exact_dot(local_onehot, group_square)
    advantage = (reward_f - sample_mean) / jnp.sqrt(sample_square - sample_mean * sample_mean + 1.0)
    seq_len = hidden.shape[0] // samp_local
    positions = jnp.arange(seq_len, dtype=jnp.int32)
    live = (positions[None, :] < lengths[:, None]).astype(jnp.float32)
    scale = (advantage[:, None] * live / lengths[:, None].astype(jnp.float32)).reshape(
        hidden.shape[0]
    )
    weighted = (cotangent.astype(jnp.float32) * scale[:, None]).astype(jnp.bfloat16)
    cols_local = cotangent.shape[1]
    block_rows = D // fsdp_size
    product = jnp.einsum("td,tc->dc", hidden, weighted, preferred_element_type=jnp.float32)
    reduced = lax.psum_scatter(
        product.reshape(1 * lax.axis_size("fsdp"), block_rows, cols_local),
        "fsdp",
        scatter_dimension=0,
        tiled=True,
    )
    owned = lax.psum_scatter(reduced, "dp", scatter_dimension=1, tiled=True)
    updated = (master - 0.1 * owned).astype(jnp.bfloat16)
    full_rows = lax.all_gather(updated, "tp", axis=2, tiled=True)
    rollout = lax.all_gather(full_rows, "dp", axis=1, tiled=True)
    return (owned, rollout)


OFFSETS = (2, 3, 1, 0)
LANES = 128
MESH = pl.DeviceIdType.MESH


def fused_kernel(
    n_dp, n_fsdp, n_tp,
    rewards_ref, groups_ref, lengths_ref, hidden_ref, cot_ref, master_ref,
    grad_ref, roll_ref,
    hid, cot, mast, cot_t, scaled, stats, mine, pair_out, pair_in, x_mine, x_out, x_in,
    z_out, z_in, mast_t, full, full_t, gathered,
    hid_sem, cot_sem, mast_sem, st_send, st_recv, m_send, m_recv, p_send, p_recv,
    x_send, x_recv, z_send, z_recv, f_send, f_recv, g_send, g_recv,
):
    dp, z, y = lax.axis_index("dp"), lax.axis_index("fsdp"), lax.axis_index("tp")
    x, c = dp // 2, dp % 2
    sibling = {"dp": x * 2 + (1 - c), "fsdp": z, "tp": y}
    x_next = {"dp": (1 - x) * 2 + c, "fsdp": z, "tp": y}
    y_next = {"dp": dp, "fsdp": z, "tp": 1 - y}
    samples = rewards_ref.shape[0]
    tokens, cols = cot.shape
    half = cols // 2
    seq = tokens // samples
    chunk = hid.shape[2]
    pair = chunk // 2
    own_rows = pair // 2

    def remote(src, dst, send, recv, where):
        return pltpu.make_async_remote_copy(
            src_ref=src, dst_ref=dst, send_sem=send, recv_sem=recv,
            device_id=where, device_id_type=MESH,
        )

    peers = [
        (i * n_fsdp + j, {"dp": (dp + i) % n_dp, "fsdp": (z + j) % n_fsdp, "tp": y})
        for i in range(n_dp) for j in range(n_fsdp) if i or j
    ]
    barrier = pltpu.get_barrier_semaphore()
    for _, where in peers:
        pl.semaphore_signal(barrier, inc=1, device_id=where, device_id_type=MESH)
    pl.semaphore_signal(barrier, inc=1, device_id=y_next, device_id_type=MESH)

    cot_copy = pltpu.make_async_copy(cot_ref, cot, cot_sem)
    cot_copy.start()
    hid_copies = []
    for k, off in enumerate(OFFSETS):
        start = pl.multiple_of(((z + off) % n_fsdp) * chunk, LANES)
        hid_copies.append(
            pltpu.make_async_copy(hidden_ref.at[:, pl.ds(start, chunk)], hid.at[k], hid_sem.at[k])
        )
        hid_copies[-1].start()
    mast_copy = pltpu.make_async_copy(master_ref.at[0], mast.at[c], mast_sem)
    mast_copy.start()

    lane = lax.broadcasted_iota(jnp.int32, (1, LANES), 1)
    total_row = jnp.zeros((1, LANES), jnp.float32)
    square_row = jnp.zeros((1, LANES), jnp.float32)
    for s in range(samples):
        reward = rewards_ref[s].astype(jnp.float32)
        hit = lane == groups_ref[s]
        total_row += jnp.where(hit, reward, 0.0)
        square_row += jnp.where(hit, reward * reward, 0.0)
    row = lax.broadcasted_iota(jnp.int32, (8, LANES), 0)
    stats[0] = jnp.where(row == 0, total_row, jnp.where(row == 1, square_row, 0.0))

    pl.semaphore_wait(barrier, len(peers) + 1)
    stat_copies = []
    for slot, where in peers:
        stat_copies.append(remote(stats.at[0], stats.at[slot], st_send.at[slot], st_recv.at[slot], where))
        stat_copies[-1].start()

    cot_copy.wait()
    cot_t[...] = cot[...].astype(jnp.float32).T
    for copy in stat_copies:
        copy.wait_recv()
    summed = stats[0]
    for slot, _ in peers:
        summed += stats[slot]
    totals, squares = summed[0:1], summed[1:2]
    for s in range(samples):
        reward = rewards_ref[s].astype(jnp.float32)
        length = lengths_ref[s]
        hit = lane == groups_ref[s]
        mean = jnp.sum(jnp.where(hit, totals, 0.0), axis=1, keepdims=True) / GROUP
        square = jnp.sum(jnp.where(hit, squares, 0.0), axis=1, keepdims=True) / GROUP
        advantage = (reward - mean) / jnp.sqrt(square - mean * mean + 1.0)
        position = lax.broadcasted_iota(jnp.int32, (1, seq), 1)
        live = jnp.where(position < length, 1.0, 0.0)
        scale = advantage * live / jnp.full((1, seq), length.astype(jnp.float32))
        at = pl.ds(s * seq, seq)
        other = cot_t[pl.ds(pl.multiple_of((1 - c) * half, 8), half), at]
        own = cot_t[pl.ds(pl.multiple_of(c * half, 8), half), at]
        scaled[0:half, at] = (other * scale).astype(jnp.bfloat16)
        scaled[half:cols, at] = (own * scale).astype(jnp.bfloat16)

    steps = len(OFFSETS)
    pair_copies = [
        remote(pair_out.at[k], pair_in.at[k], p_send.at[k], p_recv.at[k], sibling)
        for k in range(steps)
    ]
    x_copies = [
        remote(x_out.at[k], x_in.at[k], x_send.at[k], x_recv.at[k], x_next) for k in range(steps)
    ]
    z_copies = [
        remote(
            z_out.at[k], z_in.at[k], z_send.at[k], z_recv.at[k],
            {"dp": dp, "fsdp": (z + OFFSETS[k]) % n_fsdp, "tp": y},
        )
        for k in range(steps - 1)
    ]

    def multiply(k):
        hid_copies[k].wait()
        product = jnp.dot(scaled[...], hid[k], preferred_element_type=jnp.float32)
        pair_out[k] = product[0:half].astype(jnp.bfloat16)
        mine[k] = product[half:cols]
        pair_copies[k].start()

    def combine(k):
        pair_copies[k].wait_recv()
        there = pl.ds(pl.multiple_of((1 - x) * pair, LANES), pair)
        here = pl.ds(pl.multiple_of(x * pair, LANES), pair)
        x_out[k] = (mine[k, :, there] + pair_in[k, :, there].astype(jnp.float32)).astype(jnp.bfloat16)
        x_copies[k].start()
        x_mine[k] = mine[k, :, here] + pair_in[k, :, here].astype(jnp.float32)

    multiply(0)
    for k in range(1, steps):
        multiply(k)
        combine(k - 1)
    combine(steps - 1)

    mast_copy.wait()
    m_copy = remote(mast.at[c], mast.at[c], m_send, m_recv, sibling)
    m_copy.start()
    m_copy.wait_recv()
    mast_t[...] = mast[...].reshape(pair, cols).T

    for k in range(steps - 1):
        x_copies[k].wait_recv()
        z_out[k] = (x_mine[k] + x_in[k].astype(jnp.float32)).astype(jnp.bfloat16)
        z_copies[k].start()
    x_copies[steps - 1].wait_recv()
    result = x_mine[steps - 1] + x_in[steps - 1].astype(jnp.float32)
    for k in range(steps - 1):
        z_copies[k].wait_recv()
        result += z_in[k].astype(jnp.float32)
    updated = mast_t[pl.ds(pl.multiple_of(c * half, 8), half)] - 0.1 * result
    place = y * 2 + c
    gathered[x, place] = updated.astype(jnp.bfloat16)

    cut = (pair // LANES + 1) // 2 * LANES
    parts = (pl.ds(0, cut), pl.ds(cut, pair - cut))

    def spread(at_x, at_place, part, sem, where):
        ref = gathered.at[at_x, at_place, :, parts[part]]
        return remote(ref, ref, g_send.at[sem], g_recv.at[sem], where)

    y_place = (1 - y) * 2 + c
    to_x = [spread(x, place, p, p, x_next) for p in range(2)]
    to_y = [spread(x, place, p, 2 + p, y_next) for p in range(2)]
    to_sib = [spread(x, place, p, 4 + p, sibling) for p in range(2)]
    far_y = spread(1 - x, place, 0, 6, y_next)
    far_x = spread(x, y_place, 1, 7, x_next)
    relay_x = [spread(1 - x, place, p, 8 + p, sibling) for p in range(2)]
    relay_y = [spread(x, y_place, p, 10 + p, sibling) for p in range(2)]
    relay_far = [spread(1 - x, y_place, p, 12 + p, sibling) for p in range(2)]
    to_x[0].start()
    to_y[1].start()
    to_x[1].start()
    to_y[0].start()
    to_sib[0].start()
    to_sib[1].start()
    full[c] = result
    f_copy = remote(full.at[c], full.at[c], f_send, f_recv, sibling)
    f_copy.start()
    to_x[0].wait_recv()
    far_y.start()
    relay_x[0].start()
    to_y[1].wait_recv()
    far_x.start()
    relay_y[1].start()
    f_copy.wait_recv()
    full_t[...] = full[...].reshape(cols, pair).T
    grad_ref[0] = full_t[pl.ds(pl.multiple_of(c * own_rows, 8), own_rows)]
    to_x[1].wait_recv()
    relay_x[1].start()
    to_y[0].wait_recv()
    relay_y[0].start()

    def place_rows(at_x):
        rows = pl.ds(pl.multiple_of(at_x * pair, 16), pair)
        roll_ref[0, rows, :] = gathered[at_x].reshape(2 * cols, pair).T

    far_y.wait_recv()
    relay_far[0].start()
    for copy in (to_sib[0], to_sib[1], relay_y[0], relay_y[1]):
        copy.wait_recv()
    place_rows(x)
    far_x.wait_recv()
    relay_far[1].start()
    for copy in (relay_x[0], relay_x[1], relay_far[0], relay_far[1]):
        copy.wait_recv()
    place_rows(1 - x)

    sent = stat_copies + pair_copies + x_copies + z_copies + to_x + to_y + to_sib
    sent += relay_x + relay_y + relay_far + [far_y, far_x, m_copy, f_copy]
    for copy in sent:
        copy.wait_send()


def fused_shards(hidden, cotangent, rewards, groups, lengths, master):
    n_dp, n_fsdp, n_tp = lax.axis_size("dp"), lax.axis_size("fsdp"), lax.axis_size("tp")
    tokens, width = hidden.shape
    cols = cotangent.shape[1]
    half = cols // 2
    chunk = width // n_fsdp
    pair = chunk // 2
    own_rows = master.shape[1]
    steps = len(OFFSETS)
    dma, f32, bf16 = pltpu.SemaphoreType.DMA, jnp.float32, jnp.bfloat16
    smem = pl.BlockSpec(memory_space=pltpu.SMEM)
    anywhere = pl.BlockSpec(memory_space=pl.ANY)
    vmem = pl.BlockSpec(memory_space=pltpu.VMEM)
    peers = n_dp * n_fsdp
    return pl.pallas_call(
        functools.partial(fused_kernel, n_dp, n_fsdp, n_tp),
        out_shape=(
            jax.ShapeDtypeStruct((1, own_rows, cols), f32),
            jax.ShapeDtypeStruct((1, chunk, cols * n_tp), bf16),
        ),
        in_specs=[smem, smem, smem, anywhere, anywhere, anywhere],
        out_specs=(vmem, vmem),
        scratch_shapes=[
            pltpu.VMEM((steps, tokens, chunk), bf16),
            pltpu.VMEM((tokens, cols), bf16),
            pltpu.VMEM((2, own_rows, cols), f32),
            pltpu.VMEM((cols, tokens), f32),
            pltpu.VMEM((cols, tokens), bf16),
            pltpu.VMEM((peers, 8, LANES), f32),
            pltpu.VMEM((steps, half, chunk), f32),
            pltpu.VMEM((steps, half, chunk), bf16),
            pltpu.VMEM((steps, half, chunk), bf16),
            pltpu.VMEM((steps, half, pair), f32),
            pltpu.VMEM((steps, half, pair), bf16),
            pltpu.VMEM((steps, half, pair), bf16),
            pltpu.VMEM((steps, half, pair), bf16),
            pltpu.VMEM((steps, half, pair), bf16),
            pltpu.VMEM((cols, pair), f32),
            pltpu.VMEM((2, half, pair), f32),
            pltpu.VMEM((pair, cols), f32),
            pltpu.VMEM((2, 2 * n_tp, half, pair), bf16),
            dma((steps,)), dma, dma, dma((peers,)), dma((peers,)), dma, dma,
            dma((steps,)), dma((steps,)), dma((steps,)), dma((steps,)), dma((steps,)),
            dma((steps,)), dma, dma, dma((14,)), dma((14,)),
        ],
        compiler_params=pltpu.CompilerParams(
            collective_id=0, has_side_effects=True, vmem_limit_bytes=60 * 1024 * 1024
        ),
    )(rewards, groups, lengths, hidden, cotangent, master)


def fits(mesh, hidden, cotangent, rewards, groups, lengths, master):
    n_dp, n_fsdp, n_tp = mesh.shape["dp"], mesh.shape["fsdp"], mesh.shape["tp"]
    if (n_dp, n_fsdp, n_tp) != (4, len(OFFSETS), 2):
        return False
    rows_of_chip = hidden.shape[1] // n_fsdp // 2
    half = cotangent.shape[1] // n_tp // 2
    seq = hidden.shape[0] // rewards.shape[0]
    aligned = rows_of_chip % LANES == 0 and half % 16 == 0 and seq % LANES == 0
    return aligned and rewards.shape[0] // GROUP <= LANES


def solution(mesh):
    placed = (
        P(("dp", "fsdp"), None),
        P(("dp", "fsdp"), "tp"),
        P(("dp", "fsdp")),
        P(("dp", "fsdp")),
        P(("dp", "fsdp")),
        P("fsdp", "dp", "tp"),
    )

    def step(*args):
        return jax.shard_map(
            fused_shards if fits(mesh, *args) else shards,
            mesh=mesh,
            in_specs=placed,
            out_specs=(P("fsdp", "dp", "tp"), P("fsdp", None, None)),
            check_vma=False,
        )(*args)

    return step
```

```python
import functools

import jax
import jax.numpy as jnp
from jax import lax
from jax.experimental import pallas as pl
from jax.experimental.pallas import tpu as pltpu
from jax.sharding import PartitionSpec as P

D = 7168
GROUP = 16


def exact_dot(left, right):
    return jnp.dot(left, right, precision=lax.Precision.HIGHEST)


def shards(hidden, cotangent, rewards, groups, lengths, master):
    fsdp_size = lax.axis_size("fsdp")
    dp_size = lax.axis_size("dp")
    samp_local = rewards.shape[0]
    group_count = samp_local * dp_size * fsdp_size // GROUP
    labels = jnp.arange(group_count, dtype=jnp.int32)
    reward_f = rewards.astype(jnp.float32)
    local_onehot = (groups[:, None] == labels[None, :]).astype(jnp.float32)
    totals, squares = lax.psum(
        (exact_dot(reward_f, local_onehot), exact_dot(reward_f * reward_f, local_onehot)),
        ("dp", "fsdp"),
    )
    group_mean = totals / GROUP
    group_square = squares / GROUP
    sample_mean = exact_dot(local_onehot, group_mean)
    sample_square = exact_dot(local_onehot, group_square)
    advantage = (reward_f - sample_mean) / jnp.sqrt(sample_square - sample_mean * sample_mean + 1.0)
    seq_len = hidden.shape[0] // samp_local
    positions = jnp.arange(seq_len, dtype=jnp.int32)
    live = (positions[None, :] < lengths[:, None]).astype(jnp.float32)
    scale = (advantage[:, None] * live / lengths[:, None].astype(jnp.float32)).reshape(
        hidden.shape[0]
    )
    weighted = (cotangent.astype(jnp.float32) * scale[:, None]).astype(jnp.bfloat16)
    cols_local = cotangent.shape[1]
    block_rows = D // fsdp_size
    product = jnp.einsum("td,tc->dc", hidden, weighted, preferred_element_type=jnp.float32)
    reduced = lax.psum_scatter(
        product.reshape(1 * lax.axis_size("fsdp"), block_rows, cols_local),
        "fsdp",
        scatter_dimension=0,
        tiled=True,
    )
    owned = lax.psum_scatter(reduced, "dp", scatter_dimension=1, tiled=True)
    updated = (master - 0.1 * owned).astype(jnp.bfloat16)
    full_rows = lax.all_gather(updated, "tp", axis=2, tiled=True)
    rollout = lax.all_gather(full_rows, "dp", axis=1, tiled=True)
    return (owned, rollout)


STEPS = 4
LANES = 128
MESH = pl.DeviceIdType.MESH


def fused_kernel(
    n_dp, n_fsdp, n_tp,
    rewards_ref, groups_ref, lengths_ref, hidden_ref, cot_ref, master_ref,
    grad_ref, roll_ref,
    hid, cot, mast, wide, scaled, stats, mine, pair_out, pair_in, x_out, x_in,
    z_out, z_in, full, gathered,
    hid_sem, cot_sem, mast_sem, st_send, st_recv, m_send, m_recv, p_send, p_recv,
    x_send, x_recv, z_send, z_recv, f_send, f_recv, g_send, g_recv, o_sem,
):
    dp, z, y = lax.axis_index("dp"), lax.axis_index("fsdp"), lax.axis_index("tp")
    x, c = dp // 2, dp % 2
    sibling = {"dp": x * 2 + (1 - c), "fsdp": z, "tp": y}
    x_next = {"dp": (1 - x) * 2 + c, "fsdp": z, "tp": y}
    y_next = {"dp": dp, "fsdp": z, "tp": 1 - y}
    blocks = (n_fsdp - 1 - z, (z + n_fsdp // 2) % n_fsdp, z + 1 - 2 * (z % 2), z)
    samples = rewards_ref.shape[0]
    cols, tokens = cot.shape
    half = cols // 2
    seq = tokens // samples
    chunk = hid.shape[2]
    pair = chunk // 2
    own_rows = pair // 2
    cut = (pair // LANES + 1) // 2 * LANES
    parts = ((0, cut), (cut, pair - cut))
    f32, bf16 = jnp.float32, jnp.bfloat16

    def remote(src, dst, send, recv, where):
        return pltpu.make_async_remote_copy(
            src_ref=src, dst_ref=dst, send_sem=send, recv_sem=recv,
            device_id=where, device_id_type=MESH,
        )

    def side(of_x, p):
        low, wide_by = parts[p]
        return pl.ds(pl.multiple_of(of_x * pair + low, LANES), wide_by)

    def lanes(p):
        return pl.ds(*parts[p])

    peers = [
        (i * n_fsdp + j, {"dp": (dp + i) % n_dp, "fsdp": (z + j) % n_fsdp, "tp": y})
        for i in range(n_dp) for j in range(n_fsdp) if i or j
    ]
    barrier = pltpu.get_barrier_semaphore()
    for _, where in peers:
        pl.semaphore_signal(barrier, inc=1, device_id=where, device_id_type=MESH)
    pl.semaphore_signal(barrier, inc=1, device_id=y_next, device_id_type=MESH)

    cot_copy = pltpu.make_async_copy(cot_ref, cot, cot_sem)
    cot_copy.start()
    hid_copies = []
    for k in range(STEPS):
        start = pl.multiple_of(blocks[k] * chunk, LANES)
        hid_copies.append(
            pltpu.make_async_copy(hidden_ref.at[:, pl.ds(start, chunk)], hid.at[k], hid_sem.at[k])
        )
        hid_copies[-1].start()
    mast_copy = pltpu.make_async_copy(master_ref, mast.at[c], mast_sem)
    mast_copy.start()

    lane = lax.broadcasted_iota(jnp.int32, (1, LANES), 1)
    total_row = jnp.zeros((1, LANES), f32)
    square_row = jnp.zeros((1, LANES), f32)
    for s in range(samples):
        reward = rewards_ref[s].astype(f32)
        hit = lane == groups_ref[s]
        total_row += jnp.where(hit, reward, 0.0)
        square_row += jnp.where(hit, reward * reward, 0.0)
    row = lax.broadcasted_iota(jnp.int32, (8, LANES), 0)
    stats[0] = jnp.where(row == 0, total_row, jnp.where(row == 1, square_row, 0.0))

    pl.semaphore_wait(barrier, len(peers) + 1)
    stat_copies = []
    for slot, where in peers:
        stat_copies.append(remote(stats.at[0], stats.at[slot], st_send.at[slot], st_recv.at[slot], where))
        stat_copies[-1].start()

    mast_copy.wait()
    other_half = pl.ds(pl.multiple_of((1 - c) * half, 8), half)
    own_half = pl.ds(pl.multiple_of(c * half, 8), half)
    m_copy = remote(mast.at[c, other_half], mast.at[c, other_half], m_send, m_recv, sibling)
    m_copy.start()

    cot_copy.wait()
    for copy in stat_copies:
        copy.wait_recv()
    summed = stats[0]
    for slot, _ in peers:
        summed += stats[slot]
    totals, squares = summed[0:1], summed[1:2]
    for s in range(samples):
        reward = rewards_ref[s].astype(f32)
        length = lengths_ref[s]
        hit = lane == groups_ref[s]
        mean = jnp.sum(jnp.where(hit, totals, 0.0), axis=1, keepdims=True) / GROUP
        square = jnp.sum(jnp.where(hit, squares, 0.0), axis=1, keepdims=True) / GROUP
        advantage = (reward - mean) / jnp.sqrt(square - mean * mean + 1.0)
        position = lax.broadcasted_iota(jnp.int32, (1, seq), 1)
        live = jnp.where(position < length, 1.0, 0.0)
        scale = advantage * live / jnp.full((1, seq), length.astype(f32))
        at = pl.ds(s * seq, seq)
        top = (cot[0:half, at].astype(f32) * scale).astype(bf16)
        low = (cot[half:cols, at].astype(f32) * scale).astype(bf16)
        scaled[pl.ds(pl.multiple_of(c * half, 16), half), at] = low
        scaled[pl.ds(pl.multiple_of((1 - c) * half, 16), half), at] = top

    def pair_copy(k, p, at, of_x):
        ref = (k, slice(None), side(of_x, p))
        sem = (k * 2 + p) * 2 + at
        return remote(pair_out.at[ref], pair_in.at[ref], p_send.at[sem], p_recv.at[sem], sibling)

    units = [(p, k) for p in range(2) for k in range(STEPS)]
    sent = []
    pairs, x_copies, z_copies = {}, {}, {}
    for p, k in units:
        pairs[p, k] = (pair_copy(k, p, 0, 1 - x), pair_copy(k, p, 1, x))
        ref = (k, slice(None), lanes(p))
        x_copies[p, k] = remote(
            x_out.at[ref], x_in.at[ref], x_send.at[k * 2 + p], x_recv.at[k * 2 + p], x_next
        )
        sent += [*pairs[p, k], x_copies[p, k]]
        if k < STEPS - 1:
            z_copies[p, k] = remote(
                z_out.at[ref], z_in.at[ref], z_send.at[k * 2 + p], z_recv.at[k * 2 + p],
                {"dp": dp, "fsdp": blocks[k], "tp": y},
            )
            sent.append(z_copies[p, k])

    def multiply(p, k, at):
        if p == 0 and at == 0:
            hid_copies[k].wait()
        columns = side(x if at else 1 - x, p)
        product = jnp.dot(scaled[...], hid[k, :, columns], preferred_element_type=f32)
        pair_out[k, :, columns] = product[0:half].astype(bf16)
        mine[k, :, columns] = product[half:cols]
        pairs[p, k][at].start()

    def combine(p, k):
        pairs[p, k][0].wait_recv()
        columns = side(1 - x, p)
        total = mine[k, :, columns] + pair_in[k, :, columns].astype(f32)
        x_out[k, :, lanes(p)] = total.astype(bf16)
        x_copies[p, k].start()

    def reduced(p, k):
        pairs[p, k][1].wait_recv()
        columns = side(x, p)
        total = mine[k, :, columns] + pair_in[k, :, columns].astype(f32)
        x_copies[p, k].wait_recv()
        return total + x_in[k, :, lanes(p)].astype(f32)

    def forward(p, k):
        z_out[k, :, lanes(p)] = reduced(p, k).astype(bf16)
        z_copies[p, k].start()

    multiply(0, 0, 0)
    for n, (p, k) in enumerate(units):
        multiply(p, k, 1)
        if n + 1 < len(units):
            multiply(*units[n + 1], 0)
        combine(p, k)
        if n == 5:
            forward(0, 0)

    m_copy.wait_recv()
    first, second = mast[0, own_half, :], mast[1, own_half, :]
    wide[...] = jnp.concatenate([first, second], axis=1)

    place, y_place = y * 2 + c, (1 - y) * 2 + c

    def rows(at_place):
        return pl.ds(pl.multiple_of(at_place * half, 16), half)

    def spread(p, sem, at_x, at_place, where):
        ref = gathered.at[rows(at_place), side(at_x, p)]
        return remote(ref, ref, g_send.at[p * 8 + sem], g_recv.at[p * 8 + sem], where)

    def relay(p, sem, at_x, at_place):
        ref = (rows(at_place), side(at_x, p))
        return remote(
            gathered.at[ref], roll_ref.at[ref],
            g_send.at[p * 8 + sem], g_recv.at[p * 8 + sem], sibling,
        )

    def write(p, sem, at_x, at_place):
        ref = (rows(at_place), side(at_x, p))
        return pltpu.make_async_copy(gathered.at[ref], roll_ref.at[ref], o_sem.at[p * 4 + sem])

    sites = ((x, place), (1 - x, place), (x, y_place), (1 - x, y_place))
    to_x = [spread(p, 0, x, place, x_next) for p in range(2)]
    to_y = [spread(p, 1, x, place, y_next) for p in range(2)]
    far = [spread(p, 2, 1 - x, place, y_next) for p in range(2)]
    relays = [[relay(p, 3 + i, *sites[i]) for i in range(4)] for p in range(2)]
    writes = [[write(p, i, *sites[i]) for i in range(4)] for p in range(2)]
    f_copies = [
        remote(full.at[c, :, lanes(p)], full.at[c, :, lanes(p)], f_send.at[p], f_recv.at[p], sibling)
        for p in range(2)
    ]

    def finish(p):
        result = reduced(p, STEPS - 1)
        for k in range(STEPS - 1):
            z_copies[p, k].wait_recv()
            result += z_in[k, :, lanes(p)].astype(f32)
        gathered[rows(place), side(x, p)] = (wide[:, lanes(p)] - 0.1 * result).astype(bf16)
        full[c, :, lanes(p)] = result
        to_x[p].start()
        to_y[p].start()
        f_copies[p].start()
        relays[p][0].start()
        writes[p][0].start()

    def pass_on(p, i):
        relays[p][i].start()
        writes[p][i].start()

    for k in range(1, STEPS - 1):
        forward(0, k)
    forward(1, 0)
    finish(0)
    forward(1, 1)
    to_y[0].wait_recv()
    pass_on(0, 2)
    forward(1, 2)
    finish(1)
    to_x[0].wait_recv()
    far[0].start()
    pass_on(0, 1)
    for p in range(2):
        f_copies[p].wait_recv()
    for i in range(2):
        band = pl.ds(i * half, half)
        grad_ref[band, :] = jnp.where(c == 0, full[i, :, 0:own_rows], full[i, :, own_rows:pair])
    to_x[1].wait_recv()
    far[1].start()
    pass_on(1, 1)
    to_y[1].wait_recv()
    pass_on(1, 2)
    for p in range(2):
        far[p].wait_recv()
        pass_on(p, 3)

    for p in range(2):
        for i in range(4):
            relays[p][i].wait_recv()
            writes[p][i].wait()
        sent += [*relays[p], to_x[p], to_y[p], far[p], f_copies[p]]
    for copy in sent + stat_copies + [m_copy]:
        copy.wait_send()


def fused_shards(hidden, cotangent, rewards, groups, lengths, master):
    n_dp, n_fsdp, n_tp = lax.axis_size("dp"), lax.axis_size("fsdp"), lax.axis_size("tp")
    tokens, width = hidden.shape
    cols = cotangent.shape[1]
    half = cols // 2
    chunk = width // n_fsdp
    pair = chunk // 2
    own_rows = master.shape[1]
    dma, f32, bf16 = pltpu.SemaphoreType.DMA, jnp.float32, jnp.bfloat16
    smem = pl.BlockSpec(memory_space=pltpu.SMEM)
    anywhere = pl.BlockSpec(memory_space=pl.ANY)
    vmem = pl.BlockSpec(memory_space=pltpu.VMEM)
    peers = n_dp * n_fsdp
    grad, roll = pl.pallas_call(
        functools.partial(fused_kernel, n_dp, n_fsdp, n_tp),
        out_shape=(
            jax.ShapeDtypeStruct((cols, own_rows), f32),
            jax.ShapeDtypeStruct((cols * n_tp, chunk), bf16),
        ),
        in_specs=[smem, smem, smem, anywhere, anywhere, anywhere],
        out_specs=(vmem, anywhere),
        scratch_shapes=[
            pltpu.VMEM((STEPS, tokens, chunk), bf16),
            pltpu.VMEM((cols, tokens), bf16),
            pltpu.VMEM((2, cols, own_rows), f32),
            pltpu.VMEM((half, pair), f32),
            pltpu.VMEM((cols, tokens), bf16),
            pltpu.VMEM((peers, 8, LANES), f32),
            pltpu.VMEM((STEPS, half, chunk), f32),
            pltpu.VMEM((STEPS, half, chunk), bf16),
            pltpu.VMEM((STEPS, half, chunk), bf16),
            pltpu.VMEM((STEPS, half, pair), bf16),
            pltpu.VMEM((STEPS, half, pair), bf16),
            pltpu.VMEM((STEPS, half, pair), bf16),
            pltpu.VMEM((STEPS, half, pair), bf16),
            pltpu.VMEM((2, half, pair), f32),
            pltpu.VMEM((cols * n_tp, chunk), bf16),
            dma((STEPS,)), dma, dma, dma((peers,)), dma((peers,)), dma, dma,
            dma((4 * STEPS,)), dma((4 * STEPS,)), dma((2 * STEPS,)), dma((2 * STEPS,)),
            dma((2 * STEPS,)), dma((2 * STEPS,)), dma((2,)), dma((2,)), dma((16,)), dma((16,)),
            dma((8,)),
        ],
        compiler_params=pltpu.CompilerParams(
            collective_id=0, has_side_effects=True, vmem_limit_bytes=60 * 1024 * 1024
        ),
    )(rewards, groups, lengths, hidden, cotangent.T, master[0].T)
    return grad.T[None], roll.T[None]


def fits(mesh, hidden, cotangent, rewards, groups, lengths, master):
    n_dp, n_fsdp, n_tp = mesh.shape["dp"], mesh.shape["fsdp"], mesh.shape["tp"]
    if (n_dp, n_fsdp, n_tp) != (4, STEPS, 2):
        return False
    rows_of_chip = hidden.shape[1] // n_fsdp // 2
    half = cotangent.shape[1] // n_tp // 2
    seq = hidden.shape[0] // rewards.shape[0]
    aligned = rows_of_chip % LANES == 0 and half % 16 == 0 and seq % LANES == 0
    return aligned and rewards.shape[0] // GROUP <= LANES


def solution(mesh):
    placed = (
        P(("dp", "fsdp"), None),
        P(("dp", "fsdp"), "tp"),
        P(("dp", "fsdp")),
        P(("dp", "fsdp")),
        P(("dp", "fsdp")),
        P("fsdp", "dp", "tp"),
    )

    def step(*args):
        return jax.shard_map(
            fused_shards if fits(mesh, *args) else shards,
            mesh=mesh,
            in_specs=placed,
            out_specs=(P("fsdp", "dp", "tp"), P("fsdp", None, None)),
            check_vma=False,
        )(*args)

    return step
```

```python
import functools

import jax
import jax.numpy as jnp
from jax import lax
from jax.experimental import pallas as pl
from jax.experimental.pallas import tpu as pltpu
from jax.sharding import PartitionSpec as P

D = 7168
GROUP = 16


def exact_dot(left, right):
    return jnp.dot(left, right, precision=lax.Precision.HIGHEST)


def shards(hidden, cotangent, rewards, groups, lengths, master):
    fsdp_size = lax.axis_size("fsdp")
    dp_size = lax.axis_size("dp")
    samp_local = rewards.shape[0]
    group_count = samp_local * dp_size * fsdp_size // GROUP
    labels = jnp.arange(group_count, dtype=jnp.int32)
    reward_f = rewards.astype(jnp.float32)
    local_onehot = (groups[:, None] == labels[None, :]).astype(jnp.float32)
    totals, squares = lax.psum(
        (exact_dot(reward_f, local_onehot), exact_dot(reward_f * reward_f, local_onehot)),
        ("dp", "fsdp"),
    )
    group_mean = totals / GROUP
    group_square = squares / GROUP
    sample_mean = exact_dot(local_onehot, group_mean)
    sample_square = exact_dot(local_onehot, group_square)
    advantage = (reward_f - sample_mean) / jnp.sqrt(sample_square - sample_mean * sample_mean + 1.0)
    seq_len = hidden.shape[0] // samp_local
    positions = jnp.arange(seq_len, dtype=jnp.int32)
    live = (positions[None, :] < lengths[:, None]).astype(jnp.float32)
    scale = (advantage[:, None] * live / lengths[:, None].astype(jnp.float32)).reshape(
        hidden.shape[0]
    )
    weighted = (cotangent.astype(jnp.float32) * scale[:, None]).astype(jnp.bfloat16)
    cols_local = cotangent.shape[1]
    block_rows = D // fsdp_size
    product = jnp.einsum("td,tc->dc", hidden, weighted, preferred_element_type=jnp.float32)
    reduced = lax.psum_scatter(
        product.reshape(1 * lax.axis_size("fsdp"), block_rows, cols_local),
        "fsdp",
        scatter_dimension=0,
        tiled=True,
    )
    owned = lax.psum_scatter(reduced, "dp", scatter_dimension=1, tiled=True)
    updated = (master - 0.1 * owned).astype(jnp.bfloat16)
    full_rows = lax.all_gather(updated, "tp", axis=2, tiled=True)
    rollout = lax.all_gather(full_rows, "dp", axis=1, tiled=True)
    return (owned, rollout)


STEPS = 4
LANES = 128
MESH = pl.DeviceIdType.MESH


def fused_kernel(
    n_dp, n_fsdp, n_tp,
    rewards_ref, groups_ref, lengths_ref, hidden_ref, cot_ref, master_ref,
    grad_ref, roll_ref,
    hid, cot, mast, wide, scaled, stats, mine, pair_out, pair_in, x_out, x_in,
    z_out, z_in, full, gathered,
    hid_sem, cot_sem, mast_sem, st_send, st_recv, m_send, m_recv, p_send, p_recv,
    x_send, x_recv, z_send, z_recv, f_send, f_recv, g_send, g_recv, o_sem,
):
    dp, z, y = lax.axis_index("dp"), lax.axis_index("fsdp"), lax.axis_index("tp")
    x, c = dp // 2, dp % 2
    sibling = {"dp": x * 2 + (1 - c), "fsdp": z, "tp": y}
    x_next = {"dp": (1 - x) * 2 + c, "fsdp": z, "tp": y}
    y_next = {"dp": dp, "fsdp": z, "tp": 1 - y}
    blocks = (n_fsdp - 1 - z, (z + n_fsdp // 2) % n_fsdp, z + 1 - 2 * (z % 2), z)
    samples = rewards_ref.shape[0]
    cols, tokens = cot.shape
    half = cols // 2
    seq = tokens // samples
    chunk = hid.shape[2]
    pair = chunk // 2
    own_rows = pair // 2
    cut = pair // LANES * 3 // 4 * LANES
    parts = ((0, cut), (cut, pair - cut))
    f32, bf16 = jnp.float32, jnp.bfloat16

    def remote(src, dst, send, recv, where):
        return pltpu.make_async_remote_copy(
            src_ref=src, dst_ref=dst, send_sem=send, recv_sem=recv,
            device_id=where, device_id_type=MESH,
        )

    def side(of_x, p):
        low, wide_by = parts[p]
        return pl.ds(pl.multiple_of(of_x * pair + low, LANES), wide_by)

    def lanes(p):
        return pl.ds(*parts[p])

    peers = [
        (i * n_fsdp + j, {"dp": (dp + i) % n_dp, "fsdp": (z + j) % n_fsdp, "tp": y})
        for i in range(n_dp) for j in range(n_fsdp) if i or j
    ]
    barrier = pltpu.get_barrier_semaphore()
    for _, where in peers:
        pl.semaphore_signal(barrier, inc=1, device_id=where, device_id_type=MESH)
    pl.semaphore_signal(barrier, inc=1, device_id=y_next, device_id_type=MESH)

    cot_copy = pltpu.make_async_copy(cot_ref, cot, cot_sem)
    cot_copy.start()
    hid_copies = []
    for k in range(STEPS):
        start = pl.multiple_of(blocks[k] * chunk, LANES)
        hid_copies.append(
            pltpu.make_async_copy(hidden_ref.at[:, pl.ds(start, chunk)], hid.at[k], hid_sem.at[k])
        )
        hid_copies[-1].start()
    mast_copy = pltpu.make_async_copy(master_ref, mast.at[c], mast_sem)
    mast_copy.start()

    lane = lax.broadcasted_iota(jnp.int32, (1, LANES), 1)
    total_row = jnp.zeros((1, LANES), f32)
    square_row = jnp.zeros((1, LANES), f32)
    for s in range(samples):
        reward = rewards_ref[s].astype(f32)
        hit = lane == groups_ref[s]
        total_row += jnp.where(hit, reward, 0.0)
        square_row += jnp.where(hit, reward * reward, 0.0)
    row = lax.broadcasted_iota(jnp.int32, (8, LANES), 0)
    stats[0] = jnp.where(row == 0, total_row, jnp.where(row == 1, square_row, 0.0))

    pl.semaphore_wait(barrier, len(peers) + 1)
    stat_copies = []
    for slot, where in peers:
        stat_copies.append(remote(stats.at[0], stats.at[slot], st_send.at[slot], st_recv.at[slot], where))
        stat_copies[-1].start()

    mast_copy.wait()
    other_half = pl.ds(pl.multiple_of((1 - c) * half, 8), half)
    own_half = pl.ds(pl.multiple_of(c * half, 8), half)
    m_copy = remote(mast.at[c, other_half], mast.at[c, other_half], m_send, m_recv, sibling)
    m_copy.start()

    cot_copy.wait()
    for copy in stat_copies:
        copy.wait_recv()
    summed = stats[0]
    for slot, _ in peers:
        summed += stats[slot]
    totals, squares = summed[0:1], summed[1:2]
    for s in range(samples):
        reward = rewards_ref[s].astype(f32)
        length = lengths_ref[s]
        hit = lane == groups_ref[s]
        mean = jnp.sum(jnp.where(hit, totals, 0.0), axis=1, keepdims=True) / GROUP
        square = jnp.sum(jnp.where(hit, squares, 0.0), axis=1, keepdims=True) / GROUP
        advantage = (reward - mean) / jnp.sqrt(square - mean * mean + 1.0)
        position = lax.broadcasted_iota(jnp.int32, (1, seq), 1)
        live = jnp.where(position < length, 1.0, 0.0)
        scale = advantage * live / jnp.full((1, seq), length.astype(f32))
        at = pl.ds(s * seq, seq)
        top = (cot[0:half, at].astype(f32) * scale).astype(bf16)
        low = (cot[half:cols, at].astype(f32) * scale).astype(bf16)
        scaled[pl.ds(pl.multiple_of(c * half, 16), half), at] = low
        scaled[pl.ds(pl.multiple_of((1 - c) * half, 16), half), at] = top

    def pair_copy(k, p, at, of_x):
        ref = (k, slice(None), side(of_x, p))
        sem = (k * 2 + p) * 2 + at
        return remote(pair_out.at[ref], pair_in.at[ref], p_send.at[sem], p_recv.at[sem], sibling)

    units = [(p, k) for p in range(2) for k in range(STEPS)]
    sent = []
    pairs, x_copies, z_copies = {}, {}, {}
    for p, k in units:
        pairs[p, k] = (pair_copy(k, p, 0, 1 - x), pair_copy(k, p, 1, x))
        ref = (k, slice(None), lanes(p))
        x_copies[p, k] = remote(
            x_out.at[ref], x_in.at[ref], x_send.at[k * 2 + p], x_recv.at[k * 2 + p], x_next
        )
        sent += [*pairs[p, k], x_copies[p, k]]
        if k < STEPS - 1:
            z_copies[p, k] = remote(
                z_out.at[ref], z_in.at[ref], z_send.at[k * 2 + p], z_recv.at[k * 2 + p],
                {"dp": dp, "fsdp": blocks[k], "tp": y},
            )
            sent.append(z_copies[p, k])

    def multiply(p, k, at):
        if p == 0 and at == 0:
            hid_copies[k].wait()
        columns = side(x if at else 1 - x, p)
        product = jnp.dot(scaled[...], hid[k, :, columns], preferred_element_type=f32)
        pair_out[k, :, columns] = product[0:half].astype(bf16)
        mine[k, :, columns] = product[half:cols]
        pairs[p, k][at].start()

    def combine(p, k):
        pairs[p, k][0].wait_recv()
        columns = side(1 - x, p)
        total = mine[k, :, columns] + pair_in[k, :, columns].astype(f32)
        x_out[k, :, lanes(p)] = total.astype(bf16)
        x_copies[p, k].start()

    def reduced(p, k):
        pairs[p, k][1].wait_recv()
        columns = side(x, p)
        total = mine[k, :, columns] + pair_in[k, :, columns].astype(f32)
        x_copies[p, k].wait_recv()
        return total + x_in[k, :, lanes(p)].astype(f32)

    def forward(p, k):
        z_out[k, :, lanes(p)] = reduced(p, k).astype(bf16)
        z_copies[p, k].start()

    multiply(0, 0, 0)
    for n, (p, k) in enumerate(units):
        multiply(p, k, 1)
        if n + 1 < len(units):
            multiply(*units[n + 1], 0)
        combine(p, k)
        if n == 4:
            forward(0, 0)
        if n == 6:
            forward(0, 1)

    m_copy.wait_recv()
    first, second = mast[0, own_half, :], mast[1, own_half, :]
    wide[...] = jnp.concatenate([first, second], axis=1)

    place, y_place = y * 2 + c, (1 - y) * 2 + c

    def rows(at_place):
        return pl.ds(pl.multiple_of(at_place * half, 16), half)

    def spread(p, sem, at_x, at_place, where):
        ref = gathered.at[rows(at_place), side(at_x, p)]
        return remote(ref, ref, g_send.at[p * 8 + sem], g_recv.at[p * 8 + sem], where)

    def relay(p, sem, at_x, at_place):
        ref = (rows(at_place), side(at_x, p))
        return remote(
            gathered.at[ref], roll_ref.at[ref],
            g_send.at[p * 8 + sem], g_recv.at[p * 8 + sem], sibling,
        )

    def write(p, sem, at_x, at_place):
        ref = (rows(at_place), side(at_x, p))
        return pltpu.make_async_copy(gathered.at[ref], roll_ref.at[ref], o_sem.at[p * 4 + sem])

    sites = ((x, place), (1 - x, place), (x, y_place), (1 - x, y_place))
    to_x = [spread(p, 0, x, place, x_next) for p in range(2)]
    to_y = [spread(p, 1, x, place, y_next) for p in range(2)]
    far = [spread(0, 2, 1 - x, place, y_next)]
    low_lane, tail = parts[1][0], parts[1][1] // 2
    by_y = (rows(place), pl.ds(pl.multiple_of((1 - x) * pair + low_lane, LANES), tail))
    by_x = (rows(y_place), pl.ds(pl.multiple_of(x * pair + low_lane + tail, LANES), tail))
    far.append(
        remote(gathered.at[by_y], gathered.at[by_y], g_send.at[10], g_recv.at[10], y_next)
    )
    far.append(
        remote(gathered.at[by_x], gathered.at[by_x], g_send.at[7], g_recv.at[7], x_next)
    )
    relays = [[relay(p, 3 + i, *sites[i]) for i in range(4)] for p in range(2)]
    writes = [[write(p, i, *sites[i]) for i in range(4)] for p in range(2)]
    f_copies = [
        remote(full.at[c, :, lanes(p)], full.at[c, :, lanes(p)], f_send.at[p], f_recv.at[p], sibling)
        for p in range(2)
    ]

    def finish(p):
        result = reduced(p, STEPS - 1)
        for k in range(STEPS - 1):
            z_copies[p, k].wait_recv()
            result += z_in[k, :, lanes(p)].astype(f32)
        gathered[rows(place), side(x, p)] = (wide[:, lanes(p)] - 0.1 * result).astype(bf16)
        full[c, :, lanes(p)] = result
        to_x[p].start()
        to_y[p].start()
        f_copies[p].start()
        relays[p][0].start()
        writes[p][0].start()

    def pass_on(p, i):
        relays[p][i].start()
        writes[p][i].start()

    forward(0, 2)
    forward(1, 0)
    forward(1, 1)
    finish(0)
    forward(1, 2)
    to_x[0].wait_recv()
    far[0].start()
    pass_on(0, 1)
    to_y[0].wait_recv()
    pass_on(0, 2)
    finish(1)
    for p in range(2):
        f_copies[p].wait_recv()
    for i in range(2):
        band = pl.ds(i * half, half)
        grad_ref[band, :] = jnp.where(c == 0, full[i, :, 0:own_rows], full[i, :, own_rows:pair])
    to_x[1].wait_recv()
    far[1].start()
    pass_on(1, 1)
    to_y[1].wait_recv()
    far[2].start()
    pass_on(1, 2)
    far[0].wait_recv()
    pass_on(0, 3)
    far[1].wait_recv()
    far[2].wait_recv()
    pass_on(1, 3)

    for p in range(2):
        for i in range(4):
            relays[p][i].wait_recv()
            writes[p][i].wait()
        sent += [*relays[p], to_x[p], to_y[p], f_copies[p]]
    for copy in sent + far + stat_copies + [m_copy]:
        copy.wait_send()


def fused_shards(hidden, cotangent, rewards, groups, lengths, master):
    n_dp, n_fsdp, n_tp = lax.axis_size("dp"), lax.axis_size("fsdp"), lax.axis_size("tp")
    tokens, width = hidden.shape
    cols = cotangent.shape[1]
    half = cols // 2
    chunk = width // n_fsdp
    pair = chunk // 2
    own_rows = master.shape[1]
    dma, f32, bf16 = pltpu.SemaphoreType.DMA, jnp.float32, jnp.bfloat16
    smem = pl.BlockSpec(memory_space=pltpu.SMEM)
    anywhere = pl.BlockSpec(memory_space=pl.ANY)
    vmem = pl.BlockSpec(memory_space=pltpu.VMEM)
    peers = n_dp * n_fsdp
    grad, roll = pl.pallas_call(
        functools.partial(fused_kernel, n_dp, n_fsdp, n_tp),
        out_shape=(
            jax.ShapeDtypeStruct((cols, own_rows), f32),
            jax.ShapeDtypeStruct((cols * n_tp, chunk), bf16),
        ),
        in_specs=[smem, smem, smem, anywhere, anywhere, anywhere],
        out_specs=(vmem, anywhere),
        scratch_shapes=[
            pltpu.VMEM((STEPS, tokens, chunk), bf16),
            pltpu.VMEM((cols, tokens), bf16),
            pltpu.VMEM((2, cols, own_rows), f32),
            pltpu.VMEM((half, pair), f32),
            pltpu.VMEM((cols, tokens), bf16),
            pltpu.VMEM((peers, 8, LANES), f32),
            pltpu.VMEM((STEPS, half, chunk), f32),
            pltpu.VMEM((STEPS, half, chunk), bf16),
            pltpu.VMEM((STEPS, half, chunk), bf16),
            pltpu.VMEM((STEPS, half, pair), bf16),
            pltpu.VMEM((STEPS, half, pair), bf16),
            pltpu.VMEM((STEPS, half, pair), bf16),
            pltpu.VMEM((STEPS, half, pair), bf16),
            pltpu.VMEM((2, half, pair), f32),
            pltpu.VMEM((cols * n_tp, chunk), bf16),
            dma((STEPS,)), dma, dma, dma((peers,)), dma((peers,)), dma, dma,
            dma((4 * STEPS,)), dma((4 * STEPS,)), dma((2 * STEPS,)), dma((2 * STEPS,)),
            dma((2 * STEPS,)), dma((2 * STEPS,)), dma((2,)), dma((2,)), dma((16,)), dma((16,)),
            dma((8,)),
        ],
        compiler_params=pltpu.CompilerParams(
            collective_id=0, has_side_effects=True, vmem_limit_bytes=60 * 1024 * 1024
        ),
    )(rewards, groups, lengths, hidden, cotangent.T, master[0].T)
    return grad.T[None], roll.T[None]


def fits(mesh, hidden, cotangent, rewards, groups, lengths, master):
    n_dp, n_fsdp, n_tp = mesh.shape["dp"], mesh.shape["fsdp"], mesh.shape["tp"]
    if (n_dp, n_fsdp, n_tp) != (4, STEPS, 2):
        return False
    rows_of_chip = hidden.shape[1] // n_fsdp // 2
    half = cotangent.shape[1] // n_tp // 2
    seq = hidden.shape[0] // rewards.shape[0]
    aligned = rows_of_chip % (7 * LANES) == 0 and half % 16 == 0 and seq % LANES == 0
    return aligned and rewards.shape[0] // GROUP <= LANES


def solution(mesh):
    placed = (
        P(("dp", "fsdp"), None),
        P(("dp", "fsdp"), "tp"),
        P(("dp", "fsdp")),
        P(("dp", "fsdp")),
        P(("dp", "fsdp")),
        P("fsdp", "dp", "tp"),
    )

    def step(*args):
        return jax.shard_map(
            fused_shards if fits(mesh, *args) else shards,
            mesh=mesh,
            in_specs=placed,
            out_specs=(P("fsdp", "dp", "tp"), P("fsdp", None, None)),
            check_vma=False,
        )(*args)

    return step
```
